32 devices in a mesh: farcp: 4 (over z), nearcp: 4 (over y, x), tp: 2 (over core).
Axes of the slice: x: 2, y: 2, z: 4, core: 2. Of those that a mesh axis runs over, the one named last changes fastest.
Arguments:
- raw_keys: bfloat16 [16, 8192, 8, 128], P(None, ('farcp', 'nearcp'), 'tp'), may hold values from -6 to 6
- raw_values: bfloat16 [16, 8192, 8, 128], P(None, ('farcp', 'nearcp'), 'tp'), may hold values from -6 to 6
- turn_angle: float32 [8192, 64], replicated, may hold values from -3.140625 to 3.140625
Outputs:
- stored_keys: bfloat16 [16, 8192, 8, 128], P(('farcp', 'nearcp'), None, 'tp')
- stored_values: bfloat16 [16, 8192, 8, 128], P(('farcp', 'nearcp'), None, 'tp')
- key_scale: float32 [16, 8, 128], P(('farcp', 'nearcp'), 'tp')
The draws below stay inside these ranges and needn't reach their ends.
All inputs are finite; a program needn't handle non-finite values. Where the reference program divides by a largest or mean magnitude, that divisor is 1e-20 or more.
Results may differ from the reference program's by a relative error of at most 0.001.
Values may be sent and summed in bfloat16 or wider, within the bound.
A program may use at most 128 MiB of HBM per device.

```python
import jax
import jax.numpy as jnp

BATCH = 16
LENGTH = 8192
KV_HEADS = 8
HEAD_SIZE = 128
HALF_HEAD = 64


def levels(own_key, shape, cuts, low, high):
    def one(axis_at, blocks):
        steps = jax.random.uniform(jax.random.fold_in(jax.random.fold_in(own_key, 6), axis_at), (blocks,), jnp.float32, low / len(cuts), high / len(cuts))
        return jnp.repeat(jnp.exp(steps), shape[axis_at] // blocks).reshape((-1,) + (1,) * (len(shape) - axis_at - 1))

    gain = one(*cuts[0])
    for cut in cuts[1:]:
        gain = gain * one(*cut)
    return gain


def noise(stream_key, extent, scale, bound, pieces=(), kind=jnp.bfloat16):
    result = jax.random.normal(stream_key, extent, jnp.float32) * scale
    if len(pieces) > 0:
        result = levels(stream_key, extent, pieces, -0.22, 0.18) * result
    return jnp.clip(result, min=-bound, max=bound).astype(kind)


def setup_inputs(seed: int = 0) -> dict:
    arg_keys = jax.random.split(jax.random.key(seed), 4)
    return {
        "raw_keys": noise(arg_keys[0], (BATCH, LENGTH, KV_HEADS, HEAD_SIZE), 1.0, 6.0, ((1, 16), (2, 2))),
        "raw_values": noise(arg_keys[1], (BATCH, LENGTH, KV_HEADS, HEAD_SIZE), 1.0, 6.0, ((1, 16), (2, 2))),
        "turn_angle": jnp.clip(jax.random.uniform(arg_keys[2], (LENGTH, HALF_HEAD), jnp.float32, -3.140625, 3.140625), -3.140625, 3.140625),
    }


def turn_pairs(vectors, angle):
    half = vectors.shape[-1] // 2
    cosine, sine = jnp.cos(angle)[None, :, None, :], jnp.sin(angle)[None, :, None, :]
    first, second = vectors[..., :half], vectors[..., half:]
    return jnp.concatenate([first * cosine - second * sine, second * cosine + first * sine], axis=-1)


def ready_to_store(plain_keys, angle):
    wide_keys = plain_keys.astype(jnp.float32)
    return turn_pairs(wide_keys, angle)


def reference(raw_keys, raw_values, turn_angle):
    turned_keys = ready_to_store(raw_keys, turn_angle)
    key_scale = jnp.max(jnp.abs(turned_keys), axis=1)
    narrow_keys = (turned_keys / key_scale[:, None]).astype(jnp.bfloat16)
    stored_keys = narrow_keys
    stored_values = raw_values
    return stored_keys, stored_values, key_scale
```

```python
import functools

import jax
import jax.numpy as jnp
from jax import lax
from jax.experimental import pallas as pl
from jax.experimental.pallas import tpu as pltpu
from jax.sharding import PartitionSpec as P

MESH = pl.DeviceIdType.MESH


def partner_of(near, j, count):
    if count & (count - 1) == 0:
        other, bit = near, 1
        while bit < count:
            if j & bit:
                digit = lax.rem(lax.div(near, bit), 2)
                other = other + bit * (1 - 2 * digit)
            bit *= 2
        return other
    return lax.rem(2 * count - near - j, count)


def slots(count):
    return {pair: i for i, pair in enumerate((e, s) for e in range(1, count) for s in range(1, e + 1))}


def exchange_kernel(nf, nn, heads, key_in, value_in, angle, key_done, value_out, scale_out, key_side, value_side,
                    key_hold, value_hold, key_out, turned, cosines, sines, angles, scale, near_send, near_recv,
                    far_send, far_recv, own_sem, angle_sem, done_sem, scale_sem):
    f, n = lax.axis_index("farcp"), lax.axis_index("nearcp")
    me = f * nn + n
    slot = slots(nf)
    ins, outs = (key_in, value_in), (key_out, value_out)
    sides, holds = (key_side, value_side), (key_hold, value_hold)
    partners = [partner_of(n, j, nn) for j in range(nn)]

    barrier = pltpu.get_barrier_semaphore()
    for j in range(1, nn):
        pl.semaphore_signal(barrier, inc=1, device_id={"nearcp": partners[j]}, device_id_type=MESH)
    for way in (1, -1):
        @pl.when((f + way >= 0) & (f + way < nf))
        def _(way=way):
            pl.semaphore_signal(barrier, inc=1, device_id={"farcp": f + way}, device_id_type=MESH)
    pl.semaphore_wait(barrier, nn - 1 + jnp.where(f > 0, 1, 0) + jnp.where(f < nf - 1, 1, 0))

    def near_copy(t, j, r):
        d = lax.rem(f + r, nf)
        dst = outs[t].at[me] if r == 0 else sides[t].at[j - 1, d]
        i = (t * (nn - 1) + j - 1) * nf + r
        return pltpu.make_async_remote_copy(
            src_ref=ins[t].at[d * nn + partners[j]], dst_ref=dst,
            send_sem=near_send.at[i], recv_sem=near_recv.at[i],
            device_id={"nearcp": partners[j]}, device_id_type=MESH)

    def near_arrival(t, j, r):
        d = lax.rem(f + r, nf)
        dst = outs[t].at[f * nn + partners[j]] if r == 0 else sides[t].at[j - 1, d]
        i = (t * (nn - 1) + j - 1) * nf + r
        return pltpu.make_async_remote_copy(
            src_ref=dst, dst_ref=dst,
            send_sem=near_send.at[i], recv_sem=near_recv.at[i],
            device_id={"nearcp": partners[j]}, device_id_type=MESH)

    def far_copy(t, way, e, s, j):
        origin = f - way * (s - 1)
        end = origin + way * e
        active = (origin >= 0) & (origin < nf) & (end >= 0) & (end < nf)
        w = 0 if way == 1 else 1
        if s > 1:
            src = holds[t].at[w, slot[e, s - 1], j]
        elif j == 0:
            src = ins[t].at[end * nn + n]
        else:
            src = sides[t].at[j - 1, end]
        dst = outs[t].at[origin * nn + partners[j]] if s == e else holds[t].at[w, slot[e, s], j]
        i = ((t * 2 + w) * len(slot) + slot[e, s]) * nn + j
        return active, lambda: pltpu.make_async_remote_copy(
            src_ref=src, dst_ref=dst, send_sem=far_send.at[i], recv_sem=far_recv.at[i],
            device_id={"farcp": f + way}, device_id_type=MESH)

    def far_arrival(t, way, e, s, j):
        origin = f - way * s
        end = origin + way * e
        active = (origin >= 0) & (origin < nf) & (end >= 0) & (end < nf)
        w = 0 if way == 1 else 1
        dst = outs[t].at[origin * nn + partners[j]] if s == e else holds[t].at[w, slot[e, s], j]
        i = ((t * 2 + w) * len(slot) + slot[e, s]) * nn + j
        return active, lambda: pltpu.make_async_remote_copy(
            src_ref=dst, dst_ref=dst, send_sem=far_send.at[i], recv_sem=far_recv.at[i],
            device_id={"farcp": f - way}, device_id_type=MESH)

    own = [pltpu.make_async_copy(ins[t].at[me], outs[t].at[me], own_sem.at[t]) for t in range(2)]

    def first_hops(t, j):
        for e in range(nf - 1, 0, -1):
            for way in (1, -1):
                active, copy = far_copy(t, way, e, 1, j)
                @pl.when(active)
                def _(copy=copy, e=e, way=way):
                    if j > 0:
                        near_arrival(t, j, e if way == 1 else nf - e).wait_recv()
                    copy().start()

    def later_hops(t, s):
        for j in range(nn):
            for e in range(nf - 1, s - 1, -1):
                for way in (1, -1):
                    active, copy = far_copy(t, way, e, s, j)
                    _, arrival = far_arrival(t, way, e, s - 1, j)
                    @pl.when(active)
                    def _(copy=copy, arrival=arrival):
                        arrival().wait_recv()
                        copy().start()

    def final_arrivals(t):
        own[t].wait()
        for j in range(1, nn):
            near_arrival(t, j, 0).wait_recv()
        for e in range(1, nf):
            for way in (1, -1):
                for j in range(nn):
                    active, arrival = far_arrival(t, way, e, e, j)
                    @pl.when(active)
                    def _(arrival=arrival):
                        arrival().wait_recv()

    def finish_keys():
        blocks, rows, size = key_out.shape
        half = size // 2
        length = rows // heads
        group = 8
        def turn(b, top):
            place = angles[:, pl.ds(pl.multiple_of(b * length, length), length)]
            cosine, sine = jnp.cos(place), jnp.sin(place)
            cosine = jnp.concatenate([cosine, cosine], axis=0).T
            sine = jnp.concatenate([-sine, sine], axis=0).T
            for h in range(heads):
                cosines[pl.ds(h, length, stride=heads), :] = cosine
                sines[pl.ds(h, length, stride=heads), :] = sine
            piece = min(256, rows)
            def part(i, top):
                at = pl.ds(pl.multiple_of(i * piece, piece), piece)
                wide = key_out[b, at, :].astype(jnp.float32)
                y = wide * cosines[at, :] + pltpu.roll(wide, half, 1) * sines[at, :]
                turned[b, at, :] = y
                return jnp.maximum(top, jnp.max(jnp.abs(y).reshape(piece // group, group, size), axis=0))
            return lax.fori_loop(0, rows // piece, part, top)
        top = lax.fori_loop(0, blocks, turn, jnp.zeros((group, size), jnp.float32))
        biggest = top[:heads]
        for at in range(heads, group, heads):
            biggest = jnp.maximum(biggest, top[at:at + heads])
        scale[...] = biggest
        spread = jnp.concatenate([biggest] * (group // heads), axis=0)
        def narrow(b, carry):
            piece = min(256, rows)
            def part(i, carry):
                at = pl.ds(pl.multiple_of(i * piece, piece), piece)
                y = turned[b, at, :].reshape(piece // group, group, size)
                key_out[b, at, :] = (y / spread[None]).reshape(piece, size).astype(key_out.dtype)
                return carry
            lax.fori_loop(0, rows // piece, part, 0)
            pltpu.make_async_copy(key_out.at[b], key_done.at[b], done_sem.at[b]).start()
            return carry
        lax.fori_loop(0, blocks, narrow, 0)
        pltpu.make_async_copy(scale, scale_out, scale_sem).start()

    angle_copy = pltpu.make_async_copy(angle, angles, angle_sem)
    first_hops(0, 0)
    for t in range(2):
        for j in range(1, nn):
            for r in list(range(1, nf)) + [0]:
                near_copy(t, j, r).start()
    first_hops(1, 0)
    for copy in own:
        copy.start()
    angle_copy.start()
    for j in range(1, nn):
        first_hops(0, j)
    for s in range(2, nf - 1):
        later_hops(0, s)
    for j in range(1, nn):
        first_hops(1, j)
    if nf > 2:
        later_hops(0, nf - 1)
    final_arrivals(0)
    angle_copy.wait()
    finish_keys()
    for s in range(2, nf):
        later_hops(1, s)
    final_arrivals(1)
    for t in range(2):
        for j in range(1, nn):
            for r in range(nf):
                near_copy(t, j, r).wait_send()
        for (e, s) in slot:
            for way in (1, -1):
                for j in range(nn):
                    active, copy = far_copy(t, way, e, s, j)
                    @pl.when(active)
                    def _(copy=copy):
                        copy().wait_send()
    for b in range(nf * nn):
        pltpu.make_async_copy(key_out.at[b], key_done.at[b], done_sem.at[b]).wait()
    pltpu.make_async_copy(scale, scale_out, scale_sem).wait()


def exchange(nf, nn, heads, keys, values, angle):
    block = keys.shape[1:]
    k = len(slots(nf))
    out = jax.ShapeDtypeStruct(keys.shape, keys.dtype)
    side = jax.ShapeDtypeStruct((nn - 1, nf) + block, keys.dtype)
    hold = jax.ShapeDtypeStruct((2, k, nn) + block, keys.dtype)
    top = jax.ShapeDtypeStruct((heads, block[-1]), jnp.float32)
    dma = pltpu.SemaphoreType.DMA
    return pl.pallas_call(
        functools.partial(exchange_kernel, nf, nn, heads),
        out_shape=[out, out, top, side, side, hold, hold],
        in_specs=[pl.BlockSpec(memory_space=pl.ANY)] * 3,
        out_specs=[pl.BlockSpec(memory_space=pl.ANY)] * 7,
        scratch_shapes=[pltpu.VMEM(keys.shape, keys.dtype), pltpu.VMEM(keys.shape, jnp.float32),
                        pltpu.VMEM(block, jnp.float32), pltpu.VMEM(block, jnp.float32),
                        pltpu.VMEM(angle.shape, angle.dtype), pltpu.VMEM(top.shape, jnp.float32),
                        dma((2 * (nn - 1) * nf,)), dma((2 * (nn - 1) * nf,)),
                        dma((4 * k * nn,)), dma((4 * k * nn,)), dma((2,)), dma, dma((nf * nn,)), dma],
        compiler_params=pltpu.CompilerParams(
            collective_id=0, has_side_effects=True, vmem_limit_bytes=40 * 1024 * 1024),
    )(keys, values, angle)[:3]


def solution(mesh):
    nf, nn = mesh.shape["farcp"], mesh.shape["nearcp"]

    def body(raw_keys, raw_values, turn_angle):
        batch, length, heads, size = raw_keys.shape
        assert batch == nf * nn and 8 % heads == 0
        flat = (batch, length * heads, size)
        keys, values, scale = exchange(
            nf, nn, heads, raw_keys.reshape(flat), raw_values.reshape(flat), turn_angle.T)
        moved = (1, nf * nn * length, heads, size)
        return keys.reshape(moved), values.reshape(moved), scale[None]

    placed = P(None, ("farcp", "nearcp"), "tp", None)
    moved = P(("farcp", "nearcp"), None, "tp", None)
    return jax.shard_map(
        body,
        mesh=mesh,
        in_specs=(placed, placed, P()),
        out_specs=(moved, moved, P(("farcp", "nearcp"), "tp", None)),
        check_vma=False,
    )
```
